32 devices in a mesh: gz: 4 (over x, core), gx: 4 (over z), gy: 2 (over y).
Axes of the slice: x: 2, y: 2, z: 4, core: 2. Of those that a mesh axis runs over, the one named last changes fastest.
Arguments:
- offsets: float32 [3, 4, 8, 8, 128], P(None, 'gz', 'gx', 'gy'), may hold values from 0 to 10
- type_ids: int32 [4, 8, 8, 128], P('gz', 'gx', 'gy'), may hold values from 0 to 2
- occupied: int32 [4, 8, 8, 128], P('gz', 'gx', 'gy'), may hold values from 0 to 1, as said below
- prior_charges: float32 [2, 4, 8, 8, 128], P(None, 'gz', 'gx', 'gy'), may hold values from -0.6 to 0.6
- electronegativity: float32 [3], replicated, may hold values from 2 to 10
- hardness: float32 [3], replicated, may hold values from 4 to 12
- shielding: float32 [3], replicated, may hold values from 0.5 to 1.2
Outputs:
- charges: float32 [4, 8, 8, 128], P('gz', 'gx', 'gy')
- residuals: float32 [2, 4, 8, 8, 128], P(None, 'gz', 'gx', 'gy')
The draws below stay inside these ranges and needn't reach their ends.
Inputs may be any that keep to these rules, and one draw needn't show every extreme that they name: `occupied`: 1 marks a slot that holds an atom, 0 a padding slot.
All inputs are finite; a program needn't handle non-finite values.
Results may differ from the reference program's by a relative error of at most 0.00021.
Values sent between devices are 32-bit elements; how exact they have to be, the bound alone decides.
No kernel may reach another device: no remote copies, remote signals or barrier semaphores. Data moves between devices by JAX's collectives and lax.ppermute only.
A program may use at most 128 MiB of HBM per device.

```python
import jax
import jax.numpy as jnp
from jax import lax

SLOTS = 128
ITERS = 4
NTYPES = 3
NCZ = 4
NCX = 8
NCY = 8


def draw_occupied(key, part):
    shape = (NCZ, NCX, NCY, SLOTS)
    layer = jnp.arange(NCZ, dtype=jnp.int32)[:, None, None, None]
    threshold = 250 + 700 * layer // max(NCZ - 1, 1)
    rolled = jax.random.randint(jax.random.fold_in(key, 17), shape, 0, 1000)
    return (rolled < threshold).astype(jnp.int32)


def place_ends(entries, rng, smallest, high):
    place = [jax.random.randint(jax.random.fold_in(rng, axis), (), 0, length) for axis, length in enumerate(entries.shape)]
    longest = entries.shape.index(max(entries.shape))
    neighbour = place[:longest] + [(place[longest] + 1) % entries.shape[longest]] + place[longest + 1:]
    return entries.at[tuple(place)].set(smallest).at[tuple(neighbour)].set(high)


def levels(stream_key, shape, shards, least, top_value):
    def one(dim, blocks):
        heights = jax.random.uniform(jax.random.fold_in(jax.random.fold_in(stream_key, 6), dim), (blocks,), jnp.float32, least / len(shards), top_value / len(shards))
        return jnp.repeat(jnp.exp(heights), shape[dim] // blocks).reshape((-1,) + (1,) * (len(shape) - dim - 1))

    gain = one(*shards[0])
    for cut in shards[1:]:
        gain = gain * one(*cut)
    return gain


def bell_draw(stream_key, shape, deviation, limit, split=(), kind=jnp.bfloat16):
    result = jax.random.normal(stream_key, shape, jnp.float32) * deviation
    if len(split) > 0:
        result = levels(stream_key, shape, split, -0.22, 0.18) * result
    return jnp.clip(result, min=-limit, max=limit).astype(kind)


def setup_inputs(seed: int = 0) -> dict:
    streams_of = jax.random.split(jax.random.key(seed), 8)
    offsets = jnp.clip(10.0 * jax.random.uniform(streams_of[0], (3, NCZ, NCX, NCY, SLOTS), jnp.float32) ** levels(streams_of[0], (3, NCZ, NCX, NCY, SLOTS), ((1, 4), (2, 4), (3, 2)), -0.2, 0.2), 0.0, 10.0)
    type_ids = place_ends(jax.random.randint(streams_of[1], (NCZ, NCX, NCY, SLOTS), 0, NTYPES), jax.random.fold_in(streams_of[1], 1), 0, NTYPES - 1).astype(jnp.int32)
    occupied = draw_occupied(jax.random.fold_in(streams_of[7], 71), 0)
    prior_charges = bell_draw(streams_of[3], (2, NCZ, NCX, NCY, SLOTS), 0.1, 0.6, ((1, 4), (2, 4), (3, 2)), jnp.float32)
    electronegativity = jnp.clip(jax.random.uniform(streams_of[4], (NTYPES,), jnp.float32, 2.0, 10.0), 2.0, 10.0)
    hardness = jnp.clip(jax.random.uniform(streams_of[5], (NTYPES,), jnp.float32, 4.0, 12.0), 4.0, 12.0)
    shielding = jnp.clip(jax.random.uniform(streams_of[6], (NTYPES,), jnp.float32, 0.5, 1.2), 0.5, 1.2)
    return {"offsets": offsets, "type_ids": type_ids, "occupied": occupied, "prior_charges": prior_charges, "electronegativity": electronegativity, "hardness": hardness, "shielding": shielding}


coulomb_factor = 14.4
cell_edge = 10.0

def per_atom(values_table, type_ids):
    summed = jnp.zeros(type_ids.shape, jnp.float32)
    for species in range(values_table.shape[0]):
        summed = summed + jnp.where(type_ids == species, values_table[species], 0.0)
    return summed

def pair_sum(local_geo, beside, remote, shift):
    delta_z = shift[0] * cell_edge + beside[0][..., None, :] - local_geo[0][..., :, None]
    delta_x = shift[1] * cell_edge + beside[1][..., None, :] - local_geo[1][..., :, None]
    delta_y = shift[2] * cell_edge + beside[2][..., None, :] - local_geo[2][..., :, None]
    squared = delta_z * delta_z + delta_x * delta_x + delta_y * delta_y
    fraction = jnp.sqrt(squared) / cell_edge
    reach = jnp.maximum(1.0 - fraction, 0.0)
    reach = reach * reach
    taper = reach * reach * (4.0 * fraction + 1.0)
    kernel = coulomb_factor * lax.rsqrt(squared + local_geo[3][..., :, None] + beside[3][..., None, :]) * taper
    return lax.optimization_barrier(jnp.sum(kernel[None] * remote[..., None, :], axis=-1))

def couple(geometry, field):
    geo_padded = jnp.pad(geometry, ((0, 0), (1, 1), (0, 0), (0, 0), (0, 0)))
    field_padded = jnp.pad(field, ((0, 0), (1, 1), (0, 0), (0, 0), (0, 0)))

    def z_plane(index_z):
        geo_slab = lax.dynamic_slice_in_dim(geo_padded, index_z, 3, 1)
        field_slab = lax.dynamic_slice_in_dim(field_padded, index_z, 3, 1)
        local_geo = geo_slab[:, 1]
        summed = jnp.zeros((field.shape[0],) + local_geo.shape[1:], jnp.float32)
        for off_z in range(3):
            for off_x in range(3):
                for off_y in range(3):
                    beside = jnp.roll(geo_slab[:, off_z], (1 - off_x, 1 - off_y), axis=(1, 2))
                    remote = jnp.roll(field_slab[:, off_z], (1 - off_x, 1 - off_y), axis=(1, 2))
                    summed = summed + pair_sum(local_geo, beside, remote, (off_z - 1, off_x - 1, off_y - 1))
        return summed
    planes = lax.map(z_plane, jnp.arange(NCZ, dtype=jnp.int32))
    return jnp.moveaxis(planes, 0, 1)

def inner_sum(left, right):
    return lax.optimization_barrier(jnp.sum(left * right, axis=(1, 2, 3, 4)))

def expand(scalars):
    return scalars[:, None, None, None, None]

def reference(offsets, type_ids, occupied, prior_charges, electronegativity, hardness, shielding):
    occupancy = occupied.astype(jnp.float32)
    stiffness = per_atom(hardness, type_ids)
    affinity = per_atom(electronegativity, type_ids)
    radius = per_atom(shielding, type_ids)
    geometry = jnp.concatenate([offsets, (radius * radius)[None]], axis=0)

    def operate(field):
        return occupancy[None] * (stiffness[None] * field + couple(geometry, field))
    rhs = jnp.stack([-affinity * occupancy, -occupancy])
    iterate = prior_charges * occupancy[None]
    residual = rhs - operate(iterate)
    direction = residual
    norm_now = inner_sum(residual, residual)
    for iteration in range(ITERS):
        image = operate(direction)
        step_size = norm_now / inner_sum(direction, image)
        iterate = iterate + expand(step_size) * direction
        residual = residual - expand(step_size) * image
        norm_next = inner_sum(residual, residual)
        direction = residual + expand(norm_next / norm_now) * direction
        norm_now = norm_next
    totals = lax.optimization_barrier(jnp.sum(iterate, axis=(1, 2, 3, 4)))
    charges = iterate[0] - totals[0] / totals[1] * iterate[1]
    return (charges, residual)
```

```python
import functools

import jax
import jax.numpy as jnp
from jax import lax
from jax.experimental import pallas as pl
from jax.experimental.pallas import tpu as pltpu
from jax.sharding import PartitionSpec as P

ITERS = 4
AXES = ("gz", "gx", "gy")

coulomb_factor = 14.4
cell_edge = 10.0

SHIFTS = (120.0, 12.0, 60.0, 30.0)
SCALE = 64.0
PAIRS = [(i, j) for i in range(ITERS + 1) for j in range(i, ITERS + 1)]


def fill_copies(send, value, count):
    def put(i, carry):
        send[i] = value
        return carry

    lax.fori_loop(0, count, put, 0)


def typed_row(table, types, ntypes):
    row = jnp.zeros(types.shape, jnp.float32)
    for species in range(ntypes):
        row = row + jnp.where(types == species, table[species], 0.0)
    return row


def prepare(dims, devices, ntypes, en, hard, shield, offs, types, occ, prior, send, side, stage):
    lz, lx, ly = dims
    cells = lz * lx * ly
    for z in range(lz):
        for x in range(lx):
            rows = pl.ds((z * lx + x) * ly, ly)
            kinds = types[z, x]
            held = occ[z, x].astype(jnp.float32)
            for a in range(3):
                stage[a, rows, :] = offs[a, z, x]
            radius = typed_row(shield, kinds, ntypes)
            stage[3, rows, :] = radius * radius
            for s in range(2):
                stage[4 + s, rows, :] = prior[s, z, x] * held
            stiff = typed_row(hard, kinds, ntypes)
            affinity = typed_row(en, kinds, ntypes)
            for y in range(ly):
                c = (z * lx + x) * ly + y
                side[c] = stiff[y : y + 1]
                side[cells + c] = affinity[y : y + 1]
                side[2 * cells + c] = held[y : y + 1]
    fill_copies(send, stage[...], devices)


def spread(dims, near, got, groups, ext):
    lz, lx, ly = dims
    span = (lz + 2) * (lx + 2) * (ly + 2)
    for dz in range(3):
        for dx in range(3):
            for dy in range(3):
                q = (dz * 3 + dx) * 3 + dy
                source = near[q]
                valid = near[27 + q] > 0
                zs = [[lz - 1], list(range(lz)), [0]][dz]
                xs = [[lx - 1], list(range(lx)), [0]][dx]
                ys = [[ly - 1], list(range(ly)), [0]][dy]
                for dst, g in groups:
                    tile = got[source, g]
                    if dz != 1:
                        tile = jnp.where(valid, tile, 0.0)
                    for z in zs:
                        for x in xs:
                            for y in ys:
                                ez = [0, 1 + z, lz + 1][dz]
                                ex = [0, 1 + x, lx + 1][dx]
                                ey = [0, 1 + y, ly + 1][dy]
                                c = (z * lx + x) * ly + y
                                ext[dst * span + (ez * (lx + 2) + ex) * (ly + 2) + ey] = tile[c : c + 1]


def base_of(dims, c):
    lz, lx, ly = dims
    y = c % ly
    x = (c // ly) % lx
    z = c // (ly * lx)
    return (z * (lx + 2) + x) * (ly + 2) + y


def offsets_of(dims):
    lz, lx, ly = dims
    return [(dz * (lx + 2) + dx) * (ly + 2) + dy for dz in range(3) for dx in range(3) for dy in range(3)]


def build(dims, devices, near, got, side, kern, send, first, ext, column, acc, own):
    lz, lx, ly = dims
    cells = lz * lx * ly
    span = (lz + 2) * (lx + 2) * (ly + 2)
    slots = kern.shape[-1]
    c = pl.program_id(0)

    @pl.when(c == 0)
    def _():
        spread(dims, near, got, [(g, g) for g in range(6)], ext)

    base = base_of(dims, c)
    centre = base + offsets_of(dims)[13]
    for a in range(4):
        column[a] = jnp.broadcast_to(ext[a * span + centre], (slots, slots)).T
    acc[...] = jnp.zeros_like(acc)

    def one(n, carry):
        dz = n // 9
        dx = (n // 3) % 3
        dy = n % 3
        at = base + (dz * (lx + 2) + dx) * (ly + 2) + dy
        rows = []
        for a, d in enumerate((dz, dx, dy)):
            rows.append((d - 1).astype(jnp.float32) * cell_edge + ext[a * span + at])
        rad = ext[3 * span + at]
        v0 = ext[4 * span + at]
        v1 = ext[5 * span + at]
        for b in range(slots // 32):
            part = pl.ds(b * 32, 32)
            dzv = rows[0] - column[0, part, :]
            dxv = rows[1] - column[1, part, :]
            dyv = rows[2] - column[2, part, :]
            squared = dzv * dzv + dxv * dxv + dyv * dyv
            r = squared * lax.rsqrt(jnp.maximum(squared, 1e-30))
            reach = jnp.maximum(1.0 - r * (1.0 / cell_edge), 0.0)
            reach = reach * reach
            taper = reach * reach * (r * (4.0 * coulomb_factor / cell_edge) + coulomb_factor)
            k = lax.rsqrt(squared + column[3, part, :] + rad) * taper
            kern[0, n, part, :] = k
            acc[0, part, :] += k * v0
            acc[1, part, :] += k * v1
        return carry

    lax.fori_loop(0, 27, one, 0)
    stiff = side[c]
    held = side[2 * cells + c]
    for s in range(2):
        field = ext[(4 + s) * span + centre]
        total = jnp.sum(acc[s].T, axis=0, keepdims=True)
        rhs = -side[cells + c] if s == 0 else -jnp.ones_like(held)
        own[s * cells + c] = held * (rhs - (stiff * field + total))

    @pl.when(c == cells - 1)
    def _():
        for s in range(2):
            for i in range(cells):
                first[s, i : i + 1, :] = own[s * cells + i]
        fill_copies(send, first[...], devices)


def apply(dims, devices, shift, past, near, kern, got, side, *rest):
    lz, lx, ly = dims
    cells = lz * lx * ly
    span = (lz + 2) * (lx + 2) * (ly + 2)
    slots = kern.shape[-1]
    basis = rest[:past]
    if past:
        start, send, fresh, ext, acc, own, sums = rest[past:]
    else:
        send, fresh, ext, acc, own = rest
    c = pl.program_id(0)

    @pl.when(c == 0)
    def _():
        spread(dims, near, got, [(g, g) for g in range(2)], ext)

    base = base_of(dims, c)
    offs = offsets_of(dims)
    for b in range(slots // 32):
        part = pl.ds(b * 32, 32)
        a0 = jnp.zeros((32, slots), jnp.float32)
        a1 = jnp.zeros((32, slots), jnp.float32)
        for n in range(27):
            k = kern[0, n, part, :]
            a0 = a0 + k * ext[base + offs[n]]
            a1 = a1 + k * ext[span + base + offs[n]]
        acc[0, part, :] = a0
        acc[1, part, :] = a1
    stiff = side[c] - shift
    held = side[2 * cells + c]
    for s in range(2):
        field = ext[s * span + base + offs[13]]
        total = jnp.sum(acc[s].T, axis=0, keepdims=True)
        own[s * cells + c] = held * (stiff * field + total) * (1.0 / SCALE)

    @pl.when(c == cells - 1)
    def _():
        for s in range(2):
            for i in range(cells):
                fresh[s, i : i + 1, :] = own[s * cells + i]
        if past:
            sums[...] = jnp.zeros_like(sums)
            for s in range(2):
                vs = [ref[s] for ref in basis] + [fresh[s]]
                items = [vs[i] * vs[j] for i, j in PAIRS] + vs[:ITERS] + [start[near[13], 4 + s]]
                for q, item in enumerate(items):
                    sums[2 * q + s : 2 * q + s + 1, :] = jnp.sum(item, axis=0, keepdims=True)
            row = jnp.sum(sums[...].T, axis=0, keepdims=True)
            fill_copies(send, row, devices)
        else:
            fill_copies(send, fresh[...], devices)


def finish(dims, near, got, start, *rest):
    lz, lx, ly = dims
    basis = rest[: ITERS + 1]
    charges, residuals = rest[ITERS + 1 :]
    row = jnp.sum(got[...], axis=0)
    slots = row.shape[-1]
    table = jnp.broadcast_to(row, (slots, slots)).T
    pick = lambda q: table[2 * q : 2 * q + 2, :]
    gram = {}
    for q, (i, j) in enumerate(PAIRS):
        gram[i, j] = gram[j, i] = pick(q)
    sums = [pick(len(PAIRS) + k) for k in range(ITERS + 1)]
    size = ITERS + 1
    zero = jnp.zeros((2, slots), jnp.float32)

    def inner(left, right):
        total = zero
        for i in range(size):
            if left[i] is None:
                continue
            part = zero
            for j in range(size):
                if right[j] is not None:
                    part = part + gram[i, j] * right[j]
            total = total + left[i] * part
        return total

    def plus(left, scale, right):
        out = []
        for a, b in zip(left, right):
            out.append(a if b is None else scale * b if a is None else a + scale * b)
        return out

    residual = [zero + 1.0] + [None] * ITERS
    direction = list(residual)
    iterate = [None] * size
    norm_now = inner(residual, residual)
    for iteration in range(ITERS):
        image = [None] * size
        for k in range(ITERS):
            if direction[k] is not None:
                held = direction[k] * SHIFTS[k]
                image[k] = held if image[k] is None else image[k] + held
                image[k + 1] = direction[k] * SCALE
        step = norm_now / inner(direction, image)
        iterate = plus(iterate, step, direction)
        residual = plus(residual, -step, image)
        if iteration + 1 < ITERS:
            norm_next = inner(residual, residual)
            direction = plus(residual, norm_next / norm_now, direction)
            norm_now = norm_next
    totals = sums[ITERS]
    for k in range(ITERS):
        totals = totals + iterate[k] * sums[k]
    ratio = totals[0:1] / totals[1:2]
    res = []
    its = []
    for s in range(2):
        vs = [ref[s] for ref in basis]
        total = jnp.zeros_like(vs[0])
        for k in reversed(range(size)):
            total = total + residual[k][s : s + 1] * vs[k]
        res.append(total)
        total = start[near[13], 4 + s]
        for k in range(ITERS):
            total = total + iterate[k][s : s + 1] * vs[k]
        its.append(total)
    neutral = its[0] - ratio * its[1]
    for z in range(lz):
        for x in range(lx):
            first = (z * lx + x) * ly
            charges[z, x] = neutral[first : first + ly]
            for s in range(2):
                residuals[s, z, x] = res[s][first : first + ly]


def per_device(offsets, type_ids, occupied, prior_charges, electronegativity, hardness, shielding):
    dims = type_ids.shape[:3]
    lz, lx, ly = dims
    slots = type_ids.shape[3]
    cells = lz * lx * ly
    span = (lz + 2) * (lx + 2) * (ly + 2)
    ntypes = hardness.shape[0]
    nz, nx, ny = (lax.axis_size(a) for a in AXES)
    devices = nz * nx * ny
    f32 = jnp.float32
    shape = lambda *s: jax.ShapeDtypeStruct(s, f32)
    smem = pl.BlockSpec(memory_space=pltpu.SMEM)
    vmem = pl.BlockSpec(memory_space=pltpu.VMEM)
    scratch = lambda *s: pltpu.VMEM(s, f32)

    step = jnp.arange(27, dtype=jnp.int32)
    at_z = lax.axis_index("gz") + step // 9 - 1
    at_x = (lax.axis_index("gx") + (step // 3) % 3 - 1) % nx
    at_y = (lax.axis_index("gy") + step % 3 - 1) % ny
    valid = (at_z >= 0) & (at_z < nz)
    source = (jnp.clip(at_z, 0, nz - 1) * nx + at_x) * ny + at_y
    near = jnp.concatenate([source, valid.astype(jnp.int32)])

    def exchange(blocks):
        return lax.all_to_all(blocks, AXES, 0, 0, tiled=True)

    send, side = pl.pallas_call(
        functools.partial(prepare, dims, devices, ntypes),
        out_shape=(shape(devices, 6, cells, slots), shape(3 * cells, 1, slots)),
        in_specs=[smem, smem, smem, vmem, vmem, vmem, vmem],
        out_specs=(vmem, vmem),
        scratch_shapes=[scratch(6, cells, slots)],
    )(electronegativity, hardness, shielding, offsets, type_ids, occupied, prior_charges)
    start = exchange(send)
    kern_spec = pl.BlockSpec((1, 27, slots, slots), lambda c: (c, 0, 0, 0))
    kern, send, first = pl.pallas_call(
        functools.partial(build, dims, devices),
        out_shape=(shape(cells, 27, slots, slots), shape(devices, 2, cells, slots), shape(2, cells, slots)),
        grid=(cells,),
        in_specs=[smem, vmem, vmem],
        out_specs=(kern_spec, vmem, vmem),
        scratch_shapes=[
            scratch(6 * span, 1, slots),
            scratch(4, slots, slots),
            scratch(2, slots, slots),
            scratch(2 * cells, 1, slots),
        ],
    )(near, start, side)
    basis = [first]
    for k in range(ITERS):
        got = exchange(send)
        last = k + 1 == ITERS
        past = ITERS if last else 0
        extra = (*basis, start) if last else ()
        scratches = [scratch(2 * span, 1, slots), scratch(2, slots, slots), scratch(2 * cells, 1, slots)]
        if last:
            scratches.append(scratch(slots, slots))
        send, fresh = pl.pallas_call(
            functools.partial(apply, dims, devices, SHIFTS[k], past),
            out_shape=(
                shape(devices, 1, slots) if last else shape(devices, 2, cells, slots),
                shape(2, cells, slots),
            ),
            grid=(cells,),
            in_specs=[smem, kern_spec, vmem, vmem] + [vmem] * len(extra),
            out_specs=(vmem, vmem),
            scratch_shapes=scratches,
        )(near, kern, got, side, *extra)
        basis.append(fresh)
    got = exchange(send)
    return pl.pallas_call(
        functools.partial(finish, dims),
        out_shape=(shape(lz, lx, ly, slots), shape(2, lz, lx, ly, slots)),
        in_specs=[smem] + [vmem] * (ITERS + 3),
        out_specs=(vmem, vmem),
    )(near, got, start, *basis)


def solution(mesh):
    in_specs = (
        P(None, "gz", "gx", "gy", None),
        P("gz", "gx", "gy", None),
        P("gz", "gx", "gy", None),
        P(None, "gz", "gx", "gy", None),
        P(),
        P(),
        P(),
    )
    out_specs = (P("gz", "gx", "gy", None), P(None, "gz", "gx", "gy", None))
    return jax.shard_map(
        per_device, mesh=mesh, in_specs=in_specs, out_specs=out_specs, check_vma=False
    )
```
